128 devices in a mesh: rep: 1, dp: 128 (over x, y, z, core).
Axes of the slice: x: 4, y: 4, z: 4, core: 2. Of those that a mesh axis runs over, the one named last changes fastest.
Arguments:
- g_w_gate: bfloat16 [128, 2, 896, 2560], P(('rep', 'dp'))
- g_w_up: bfloat16 [128, 2, 896, 2560], P(('rep', 'dp'))
- g_w_down: bfloat16 [128, 2, 2560, 896], P(('rep', 'dp'))
- w_gate: bfloat16 [2, 896, 2560], replicated
- w_up: bfloat16 [2, 896, 2560], replicated
- w_down: bfloat16 [2, 2560, 896], replicated
- m_w_gate: float32 [2, 896, 2560], P(None, 'dp')
- m_w_up: float32 [2, 896, 2560], P(None, 'dp')
- m_w_down: float32 [2, 2560, 896], P(None, 'dp')
- v_w_gate: float32 [2, 896, 2560], P(None, 'dp')
- v_w_up: float32 [2, 896, 2560], P(None, 'dp')
- v_w_down: float32 [2, 2560, 896], P(None, 'dp')
Outputs:
- output 1: bfloat16 [2, 896, 2560], P('rep')
- output 2: bfloat16 [2, 896, 2560], P('rep')
- output 3: bfloat16 [2, 2560, 896], P('rep')
- output 4: float32 [2, 896, 2560], P('rep', 'dp')
- output 5: float32 [2, 896, 2560], P('rep', 'dp')
- output 6: float32 [2, 2560, 896], P('rep', 'dp')
- output 7: float32 [2, 896, 2560], P('rep', 'dp')
- output 8: float32 [2, 896, 2560], P('rep', 'dp')
- output 9: float32 [2, 2560, 896], P('rep', 'dp')
All inputs are finite; a program needn't handle non-finite values.
Results may differ from the reference program's by a relative error of at most 0.022.
Values are sent between devices in bfloat16 or wider.
A program may use at most 1.5 GiB of HBM per device.

```python
import jax
import jax.numpy as jnp
from jax import lax

DEVICES = 128
D = 896
FF = 2560
LAYERS = 2
NAMES = ("w_gate", "w_up", "w_down")
SHAPES = {"w_gate": (LAYERS, D, FF), "w_up": (LAYERS, D, FF), "w_down": (LAYERS, FF, D)}


def setup_inputs(seed: int = 0, part: int = 0) -> dict:
    kz, *keys = jax.random.split(jax.random.key(seed), 1 + 5 * len(NAMES))
    loud = 2.0 ** jax.random.uniform(kz, (), jnp.float32, -1.0, 1.0)
    drawn = {}
    for name, key, both in zip(NAMES, keys[:3], keys[3:6], strict=True):
        own = jax.random.normal(jax.random.fold_in(key, part), (DEVICES, *SHAPES[name]), jnp.float32)
        shared = jax.random.normal(jax.random.fold_in(both, part), SHAPES[name], jnp.float32)
        drawn["g_" + name] = (loud * (0.7 * shared / DEVICES + 0.7 * own * DEVICES**-0.5)).astype(jnp.bfloat16)
    for name, key in zip(NAMES, keys[6:9], strict=True):
        drawn[name] = (jax.random.normal(key, SHAPES[name], jnp.float32) * SHAPES[name][1] ** -0.5).astype(jnp.bfloat16)
    for name, key in zip(NAMES, keys[9:12], strict=True):
        drawn["m_" + name] = loud * 0.5 * jax.random.normal(key, SHAPES[name], jnp.float32)
    for name, key in zip(NAMES, keys[12:15], strict=True):
        drawn["v_" + name] = loud * loud * jax.random.uniform(key, SHAPES[name], jnp.float32, 0.5, 1.5)
    return drawn


def adamw(w, m, v, g):
    m = 0.9 * m + 0.1 * g
    v = 0.95 * v + 0.05 * g * g
    step = m * lax.rsqrt(v + 1e-8) + 0.1 * w
    return (w - 0.02 * step).astype(jnp.bfloat16), m, v


def clipped(gradients, sum_of_squares, count):
    factor = jnp.minimum(1.0, 0.5 * lax.rsqrt(sum_of_squares / count + 1e-30))
    return [g * factor for g in gradients]


def reference(g_w_gate, g_w_up, g_w_down, w_gate, w_up, w_down, m_w_gate, m_w_up, m_w_down, v_w_gate, v_w_up, v_w_down):
    def total(terms):
        return lax.scan(lambda so_far, term: (so_far + term.astype(jnp.float32), None), jnp.zeros(terms.shape[1:], jnp.float32), terms)[0]

    gradients = [total(terms).astype(jnp.bfloat16).astype(jnp.float32) for terms in (g_w_gate, g_w_up, g_w_down)]
    gradients = clipped(gradients, sum(jnp.sum(g * g) for g in gradients), sum(g.size for g in gradients))
    new = [
        adamw(w.astype(jnp.float32), m, v, g)
        for w, m, v, g in zip((w_gate, w_up, w_down), (m_w_gate, m_w_up, m_w_down), (v_w_gate, v_w_up, v_w_down), gradients, strict=True)
    ]
    return tuple(one[which] for which in range(3) for one in new)
```

```python
import functools

import jax
import jax.numpy as jnp
from jax import lax
from jax.experimental import pallas as pl
from jax.experimental.pallas import tpu as pltpu
from jax.sharding import PartitionSpec as P

MESH = pl.DeviceIdType.MESH
F32, BF16 = jnp.float32, jnp.bfloat16
X, Y, Z = 0, 1, 2
RIGHT, LEFT = 0, 1
PLAIN, DOWN = (0, 1), (2, 3)
GROUP, OTHERS, STEPS = range(8), range(1, 8), (1, 2, 3)
VMEM_LIMIT = 60 * 2**20


def div(a, n):
    return lax.div(a, jnp.int32(n))


def rem(a, n):
    return lax.rem(a, jnp.int32(n))


class Place:
    def __init__(self):
        i = lax.axis_index("dp")
        self.c = rem(i, 2)
        self.at = (div(i, 32), rem(div(i, 8), 4), rem(div(i, 2), 4))
        self.j = rem(i, 8)

    def device(self, at, c):
        return {"dp": ((at[0] * 4 + at[1]) * 4 + at[2]) * 2 + c}

    def along(self, axis, by):
        to = rem(self.at[axis] + (by + 4), 4)
        at = tuple(to if a == axis else v for a, v in enumerate(self.at))
        return self.device(at, self.c), to

    def partner(self):
        return self.device(self.at, 1 - self.c)

    def group(self, by):
        j = rem(self.j + by, 8)
        return self.device((self.at[0], self.at[1], div(j, 2)), rem(j, 2)), j

    def barrier(self):
        sem = pltpu.get_barrier_semaphore()
        peers = [self.along(a, by)[0] for a in (X, Y) for by in STEPS] + [self.group(by)[0] for by in OTHERS]
        for d in peers:
            pl.semaphore_signal(sem, inc=1, device_id=d, device_id_type=MESH)
        pl.semaphore_wait(sem, len(peers))


class Job:
    def __init__(self, mat, order, rows, c0, c1):
        self.mat, self.order, self.rows, self.c0, self.c1 = mat, order, rows, c0, c1
        self.cols = c1 - c0
        self.axes = tuple(sorted(order))
        self.rings = 2

    def rest(self, p):
        return tuple(sorted(self.order[p + 1 :]))

    def block_shape(self, p):
        return (4,) * len(self.rest(p)) + (self.rows, self.cols)

    def unit_shape(self, p):
        rest = self.rest(p)
        if not rest:
            return (self.rows, self.cols // 2)
        return tuple(2 if a == self.order[-1] else 4 for a in rest) + (self.rows, self.cols)

    def unit(self, place, p, blk, h):
        co = {a: place.at[a] for a in self.order[:p]}
        co[self.order[p]] = blk
        for a in self.order[p + 1 :]:
            co[a] = pl.ds(0, 4)
        cols = (0, self.cols)
        if self.order[p + 1 :]:
            co[self.order[-1]] = pl.ds(2 * h, 2)
        elif h is not None:
            cols = (h * (self.cols // 2), (h + 1) * (self.cols // 2))
        return co, cols

    def whole(self, ref, unit, lead=()):
        co, (lo, hi) = unit
        return ref.at[(*lead, *(co[a] for a in self.axes), slice(None), pl.ds(self.c0 + lo, hi - lo))]

    def part(self, ref, p, side, unit):
        co, (lo, hi) = unit
        return ref.at[(side, *(co[a] for a in self.rest(p)), slice(None), pl.ds(lo, hi - lo))]


def jobs_of(shape_gate, shape_down):
    cols, down = shape_gate[-1], shape_down[-1]
    cut = (down // 128 + 1) // 2 * 128
    return (
        Job(0, (X, Y), shape_gate[-2], 0, cols),
        Job(1, (Y, X), shape_gate[-2], 0, cols),
        Job(2, (Z, X, Y), shape_down[-2], 0, cut),
        Job(2, (Z, Y, X), shape_down[-2], cut, down),
    )


def add_up(dst, srcs):
    *lead, rows, _ = dst.shape
    tiles = rows // 8
    count = tiles
    for d in lead:
        count *= d

    def body(i, _):
        at, up = [], div(i, tiles)
        for d in reversed(lead):
            at.append(rem(up, d))
            up = div(up, d)
        ix = (*reversed(at), pl.ds(pl.multiple_of(rem(i, tiles) * 8, 8), 8), slice(None))
        total = srcs[0][ix].astype(F32)
        for s in srcs[1:]:
            total = total + s[ix].astype(F32)
        dst[ix] = total.astype(dst.dtype)
        return 0

    lax.fori_loop(0, count, body, 0)


def reduce_kernel(jobs, g0, g1, g2, o0, o1, o2, osq, *s):
    s = list(s)
    take = lambda n: [s.pop(0) for _ in range(n)]
    hbm = (g0, g1, g2)
    mine, theirs = take(3), take(3)
    ra = [take(2) for _ in jobs]
    rb = [take(2) for _ in jobs]
    r3 = take(2)
    summed, pieces, got = take(3), take(2), take(2)
    piece_d, got_d = take(2)
    total, total_d, squares = take(3)
    load_sem, d2d_send, d2d_recv, ring_send, ring_recv, end_send, end_recv, third_send, third_recv, sq_send, sq_recv, down_send, down_recv = take(13)

    me = Place()
    me.barrier()
    c = me.c

    kinds = [(2, 0), (2, 1), (1, 1), (-1, 0), (1, 0), (-1, 1), (0, 0), (0, 1)]
    loads, swaps = {}, {}
    for k, (by, h) in enumerate(kinds):
        for n, job in enumerate(jobs):
            _, blk = me.along(job.order[0], by)
            unit = job.unit(me, 0, blk, h)
            swaps[n, k] = pltpu.make_async_remote_copy(
                job.whole(hbm[job.mat], unit, (1 - c,)), job.whole(theirs[job.mat], unit),
                d2d_send.at[n, k], d2d_recv.at[n, k], device_id=me.partner(), device_id_type=MESH)
            loads[n, k] = pltpu.make_async_copy(job.whole(hbm[job.mat], unit, (c,)), job.whole(mine[job.mat], unit), load_sem.at[n, k])
            swaps[n, k].start()
            loads[n, k].start()

    sent = []

    def terms(n, p, unit):
        job = jobs[n]
        refs = [job.whole(mine[job.mat], unit), job.whole(theirs[job.mat], unit)]
        for q in range(p):
            refs += [job.part(rb[n][q], q, side, unit) for side in (0, 1)]
        return refs

    def send(n, p, kind):
        job, way = jobs[n], kind % 2
        axis = job.order[p]
        to, _ = me.along(axis, 1 if way == RIGHT else -1)
        by, h = kinds[kind]
        _, blk = me.along(axis, by)
        unit = job.unit(me, p, blk, h)
        if p == 0:
            loads[n, kind].wait()
            swaps[n, kind].wait_recv()
        refs = terms(n, p, unit)
        if kind >= 4:
            ring[n, p, way].wait_recv()
            refs.append(ra[n][p].at[way])
        add_up(refs[0], refs)
        _, own = me.along(axis, 0)
        into = ra[n][p].at[way] if kind < 2 else job.part(rb[n][p], p, way, job.unit(me, p, own, h))
        ring[n, p, kind] = pltpu.make_async_remote_copy(
            refs[0], into, ring_send.at[n, p, kind], ring_recv.at[n, p, kind], device_id=to, device_id_type=MESH)
        ring[n, p, kind].start()
        sent.append(ring[n, p, kind])

    ring = {}
    for kind in range(6):
        for n in range(len(jobs)):
            send(n, 0, kind)
    for kind in (6, 7):
        for n in range(len(jobs)):
            loads[n, kind].wait()
            swaps[n, kind].wait_recv()
    for n in range(len(jobs)):
        for kind in range(2, 6):
            ring[n, 0, kind].wait_recv()
        for kind in range(4):
            send(n, 1, kind)
    for n in range(len(jobs)):
        for kind in (4, 5):
            send(n, 1, kind)

    for n in DOWN:
        job = jobs[n]
        for kind in range(2, 6):
            ring[n, 1, kind].wait_recv()
        for by in STEPS:
            to, blk = me.along(job.order[2], by)
            refs = terms(n, 2, job.unit(me, 2, blk, None))
            add_up(refs[0], refs)
            ring[n, 2, by] = pltpu.make_async_remote_copy(
                refs[0], r3[n - 2].at[by - 1], third_send.at[n - 2, by - 1], third_recv.at[n - 2, by - 1], device_id=to, device_id_type=MESH)
            ring[n, 2, by].start()
            sent.append(ring[n, 2, by])

    last = {}
    for n in PLAIN:
        job = jobs[n]
        for kind in range(2, 6):
            ring[n, 1, kind].wait_recv()
        unit = ({a: me.at[a] for a in job.axes}, (0, job.cols))
        refs = terms(n, 2, unit)
        add_up(summed[n].at[pl.ds(0, job.rows)], refs)
        summed[n][pl.ds(job.rows, 8), :] = jnp.zeros((8, job.cols), F32)
        for j in GROUP:
            pieces[n][j] = summed[n][7 * j : 7 * j + 8, :].astype(BF16)
        for by in OTHERS:
            to, j = me.group(by)
            last[n, by] = pltpu.make_async_remote_copy(
                pieces[n].at[j], got[n].at[me.j], end_send.at[n, by], end_recv.at[n, by], device_id=to, device_id_type=MESH)
            last[n, by].start()
            sent.append(last[n, by])
        got[n][me.j] = jnp.zeros(got[n].shape[1:], BF16)
        for j in GROUP:
            @pl.when(me.j == j)
            def _(j=j, n=n):
                total[n, c] = summed[n][7 * j : 7 * j + 8, :]
        total[n, 1 - c] = jnp.zeros(total.shape[2:], F32)

    rows = jobs[2].rows
    half = rows // 2
    for n in DOWN:
        job = jobs[n]
        for by in STEPS:
            ring[n, 2, by].wait_recv()
        unit = ({a: me.at[a] for a in job.axes}, (0, job.cols))
        refs = terms(n, 2, unit) + [r3[n - 2].at[k] for k in range(3)]
        add_up(summed[2].at[pl.ds(0, rows), pl.ds(job.c0, job.cols)], refs)
    summed[2][pl.ds(rows, 8), :] = jnp.zeros((8, summed[2].shape[1]), F32)
    pad = piece_d.shape[0]
    for k in range(2):
        @pl.when(c == k)
        def _(k=k):
            total_d[c] = summed[2][half * k : half * k + pad, :]
            piece_d[...] = summed[2][half * (1 - k) : half * (1 - k) + pad, :].astype(BF16)
    down = pltpu.make_async_remote_copy(piece_d, got_d, down_send, down_recv, device_id=me.partner(), device_id_type=MESH)
    down.start()
    sent.append(down)

    keep = lax.broadcasted_iota(jnp.int32, (8, 1), 0) < 7
    square = jnp.zeros((8, total.shape[-1]), F32)
    for n, out in ((0, o0), (1, o1)):
        for by in OTHERS:
            last[n, by].wait_recv()
        for layer in range(2):
            t = total[n, layer]
            for z in range(4):
                t = t + got[n][2 * z + layer].astype(F32)
            t = t.astype(BF16)
            out[layer] = t
            t = jnp.where(keep, t.astype(F32), 0.0)
            square = square + t * t
    square_d = jnp.zeros((8, total_d.shape[-1]), F32)
    down.wait_recv()
    total_d[1 - c] = got_d[...].astype(F32)
    for layer in range(2):
        for r in range(0, half, 8):
            t = total_d[layer, r : r + 8].astype(BF16)
            o2[layer, r : r + 8] = t
            t = t.astype(F32)
            if half - r < 8:
                t = jnp.where(lax.broadcasted_iota(jnp.int32, (8, 1), 0) < half - r, t, 0.0)
            square_d = square_d + t * t
    lanes = jnp.zeros((8, 128), F32)
    for k in range(0, square.shape[1], 128):
        lanes = lanes + square[:, k : k + 128]
    for k in range(0, square_d.shape[1], 128):
        lanes = lanes + square_d[:, k : k + 128]

    for step, (size, own) in enumerate(((4, me.at[0]), (4, me.at[1]), (8, me.j))):
        squares[step, own] = lanes
        copies = []
        for by in range(1, size):
            to = me.group(by)[0] if step == 2 else me.along(step, by)[0]
            copies.append(pltpu.make_async_remote_copy(
                squares.at[step, own], squares.at[step, own], sq_send.at[step, by], sq_recv.at[step, by], device_id=to, device_id_type=MESH))
            copies[-1].start()
        sent.extend(copies)
        for copy in copies:
            copy.wait_recv()
        lanes = squares[step, 0]
        for k in range(1, size):
            lanes = lanes + squares[step, k]
    osq[...] = lanes

    for copy in sent:
        copy.wait_send()
    for copy in swaps.values():
        copy.wait_send()


def gather_kernel(jobs, n0, n1, n2, o0, o1, o2, *s):
    s = list(s)
    take = lambda n: [s.pop(0) for _ in range(n)]
    outs = (o0, o1, o2)
    new = (n0, n1, n2)
    whole = take(3)
    pieces, piece_d, summed = take(2), *take(1), take(3)
    end_send, end_recv, down_send, down_recv, third_send, third_recv, ring_send, ring_recv, out_sem, d2d_send, d2d_recv = take(11)

    me = Place()
    me.barrier()
    c = me.c
    sent = []

    def go(copy):
        copy.start()
        sent.append(copy)
        return copy

    last = {}
    for n in PLAIN:
        for by in OTHERS:
            to, j = me.group(by)
            last[n, by] = go(pltpu.make_async_remote_copy(
                new[n].at[rem(j, 2)], pieces[n].at[me.j], end_send.at[n, by], end_recv.at[n, by], device_id=to, device_id_type=MESH))
        pieces[n][me.j] = new[n][c]
    down = go(pltpu.make_async_remote_copy(new[2].at[1 - c], piece_d.at[c], down_send, down_recv, device_id=me.partner(), device_id_type=MESH))
    piece_d[c] = new[2][c]

    rows = jobs[2].rows
    half, pad = rows // 2, piece_d.shape[1]
    down.wait_recv()
    for k in range(2):
        summed[2][half * k : half * k + pad, :] = piece_d[k].astype(F32)
    mat = whole[2].at[me.at]
    for r in range(0, rows, 8):
        mat[r : r + 8, :] = summed[2][r : r + 8, :].astype(BF16)
    third = {}
    for n in DOWN:
        job = jobs[n]
        ref = job.whole(whole[2], ({a: me.at[a] for a in job.axes}, (0, job.cols)))
        for by in STEPS:
            to, _ = me.along(job.order[2], by)
            third[n, by] = go(pltpu.make_async_remote_copy(ref, ref, third_send.at[n - 2, by], third_recv.at[n - 2, by], device_id=to, device_id_type=MESH))

    for n in PLAIN:
        job = jobs[n]
        for by in OTHERS:
            last[n, by].wait_recv()
        for j in GROUP:
            summed[n][7 * j : 7 * j + 8, :] = pieces[n][j].astype(F32)
        mat = whole[n].at[me.at[:2]]
        for r in range(0, job.rows, 8):
            mat[r : r + 8, :] = summed[n][r : r + 8, :].astype(BF16)

    ring = {}

    def send(n, p, kind):
        job, way = jobs[n], kind % 2
        to, _ = me.along(job.order[p], 1 if way == RIGHT else -1)
        by, h = ((0, 0), (0, 1), (0, 1), (0, 0), (-1, 0), (1, 1))[kind]
        _, blk = me.along(job.order[p], by)
        if kind >= 4:
            ring[n, p, way].wait_recv()
        ref = job.whole(whole[job.mat], job.unit(me, p, blk, h))
        ring[n, p, kind] = go(pltpu.make_async_remote_copy(
            ref, ref, ring_send.at[n, p, kind], ring_recv.at[n, p, kind], device_id=to, device_id_type=MESH))

    writes, swaps = [], []

    def put(n, k, by, h):
        job = jobs[n]
        _, blk = me.along(job.order[0], by)
        unit = job.unit(me, 0, blk, h)
        src, dst = job.whole(whole[job.mat], unit), job.whole(outs[job.mat], unit, (c,))
        swaps.append(go(pltpu.make_async_remote_copy(src, dst, d2d_send.at[n, k], d2d_recv.at[n, k], device_id=me.partner(), device_id_type=MESH)))
        writes.append(pltpu.make_async_copy(src, dst, out_sem.at[n, k]))
        writes[-1].start()

    order = (2, 3, 0, 1)
    for n in order:
        if n >= 2:
            for by in STEPS:
                third[n, by].wait_recv()
        for kind in range(4):
            send(n, 1, kind)
    for n in order:
        for kind in (4, 5):
            send(n, 1, kind)
    for n in order:
        for kind in range(2, 6):
            ring[n, 1, kind].wait_recv()
        for kind in range(4):
            send(n, 0, kind)
        for h in (0, 1):
            put(n, 6 + h, 0, h)
    came = ((-1, 0), (1, 1), (-1, 1), (1, 0), (2, 0), (2, 1))
    for kind in (4, 5):
        for n in order:
            send(n, 0, kind)
            put(n, kind - 4, *came[kind - 4])
    for kind in range(2, 6):
        for n in order:
            ring[n, 0, kind].wait_recv()
            put(n, kind, *came[kind])
    for copy in swaps:
        copy.wait_recv()
    for copy in writes:
        copy.wait()
    for copy in sent:
        copy.wait_send()


def adamw(w, m, v, g):
    m = 0.9 * m + 0.1 * g
    v = 0.95 * v + 0.05 * g * g
    step = m * lax.rsqrt(v + 1e-8) + 0.1 * w
    return (w - 0.02 * step).astype(BF16), m, v


def dma(*shape):
    return pltpu.SemaphoreType.DMA(shape) if shape else pltpu.SemaphoreType.DMA


def reduce_call(jobs, *g):
    cols, down, rows = g[0].shape[-1], g[2].shape[-1], jobs[2].rows
    pad = rows // 2 + 4
    mats = [pltpu.VMEM(x.shape[1:], BF16) for x in g]
    scratch = mats + mats
    for job in jobs:
        scratch += [pltpu.VMEM((2, *job.unit_shape(p)), BF16) for p in range(2)]
    for job in jobs:
        scratch += [pltpu.VMEM((2, *job.block_shape(p)), BF16) for p in range(2)]
    scratch += [pltpu.VMEM((3, rows, job.cols), BF16) for job in jobs[2:]]
    scratch += [pltpu.VMEM((jobs[0].rows + 8, cols), F32)] * 2 + [pltpu.VMEM((rows + 8, down), F32)]
    scratch += [pltpu.VMEM((8, 8, cols), BF16)] * 4
    scratch += [pltpu.VMEM((pad, down), BF16)] * 2
    scratch += [pltpu.VMEM((2, 2, 8, cols), F32), pltpu.VMEM((2, pad, down), F32), pltpu.VMEM((3, 8, 8, 128), F32)]
    n = len(jobs)
    scratch += [dma(n, 8)] * 3 + [dma(n, 2, 6)] * 2 + [dma(2, 8)] * 2 + [dma(2, 3)] * 2 + [dma(3, 8)] * 2 + [dma()] * 2
    return pl.pallas_call(
        functools.partial(reduce_kernel, jobs),
        out_shape=[jax.ShapeDtypeStruct((2, 8, cols), BF16)] * 2 + [jax.ShapeDtypeStruct((2, pad, down), BF16), jax.ShapeDtypeStruct((8, 128), F32)],
        in_specs=[pl.BlockSpec(memory_space=pl.ANY)] * 3,
        out_specs=[pl.BlockSpec(memory_space=pltpu.VMEM)] * 4,
        scratch_shapes=scratch,
        compiler_params=pltpu.CompilerParams(collective_id=0, has_side_effects=True, vmem_limit_bytes=VMEM_LIMIT),
        name="reduce",
    )(*g)


def gather_call(jobs, shapes, *new):
    cols, (pad, down), rows = new[0].shape[-1], new[2].shape[1:], jobs[2].rows
    scratch = [pltpu.VMEM(s, BF16) for s in shapes]
    scratch += [pltpu.VMEM((8, 8, cols), BF16)] * 2 + [pltpu.VMEM((2, pad, down), BF16)]
    scratch += [pltpu.VMEM((jobs[0].rows + 8, cols), F32)] * 2 + [pltpu.VMEM((rows + 8, down), F32)]
    n = len(jobs)
    scratch += [dma(2, 8)] * 2 + [dma()] * 2 + [dma(2, 4)] * 2 + [dma(n, 2, 6)] * 2 + [dma(n, 8)] * 3
    return pl.pallas_call(
        functools.partial(gather_kernel, jobs),
        out_shape=[jax.ShapeDtypeStruct((2, *s), BF16) for s in shapes],
        in_specs=[pl.BlockSpec(memory_space=pltpu.VMEM)] * 3,
        out_specs=[pl.BlockSpec(memory_space=pl.ANY)] * 3,
        scratch_shapes=scratch,
        compiler_params=pltpu.CompilerParams(collective_id=1, has_side_effects=True, vmem_limit_bytes=VMEM_LIMIT),
        name="gather",
    )(*new)


def solution(mesh):
    def step(*arrays):
        terms, weights, m, v = (arrays[i : i + 3] for i in (0, 3, 6, 9))
        full = [w.shape for w in weights]
        shapes = [(4, 4, full[0][1] // 16, full[0][2])] * 2 + [(4, 4, 4, full[2][1] // 64, full[2][2])]
        jobs = jobs_of(shapes[0], shapes[2])
        *sums, squares = reduce_call(jobs, *(t.reshape(2, *s) for t, s in zip(terms, shapes, strict=True)))
        factor = jnp.minimum(1.0, 0.5 * lax.rsqrt(jnp.sum(squares) / (128 * sum(one.size for one in m)) + 1e-30))
        me = lax.axis_index("dp")
        new = []
        for w, mm, vv, g in zip(weights, m, v, sums, strict=True):
            rows = mm.shape[1]
            own = lax.dynamic_slice_in_dim(w, me * rows, rows, 1).astype(F32)
            new.append(adamw(own, mm, vv, g[:, :rows].astype(F32) * factor))
        padded = [jnp.pad(one[0], ((0, 0), (0, g.shape[1] - one[0].shape[1]), (0, 0))) for one, g in zip(new, sums, strict=True)]
        whole = gather_call(jobs, shapes, *padded)
        whole = [w.reshape(s) for w, s in zip(whole, full, strict=True)]
        return (*whole, *(one[1] for one in new), *(one[2] for one in new))

    all_of, cut = P(None, None, None), P(None, "dp", None)
    return jax.shard_map(
        step,
        mesh=mesh,
        in_specs=(P(("rep", "dp"), None, None, None),) * 3 + (all_of,) * 3 + (cut,) * 6,
        out_specs=(P("rep", None, None),) * 3 + (P("rep", "dp", None),) * 6,
        check_vma=False,
    )
```
